16 devices in a mesh: dp: 2 (over y, z), tp: 8 (over x, core).
Axes of the slice: x: 4, y: 2, z: 1, core: 2. Of those that a mesh axis runs over, the one named last changes fastest.
The devices are a block of a 4x4x8 slice.
Arguments:
- x: bfloat16 [8, 512, 8192], P('dp'), parts along dimension 0
- gain_a: bfloat16 [8192], replicated
- wq: bfloat16 [8192, 8192], P(None, 'tp')
- wk: bfloat16 [8192, 8192], P(None, 'tp')
- wv: bfloat16 [8192, 8192], P(None, 'tp')
- wo: bfloat16 [8192, 8192], P('tp')
- gain_m: bfloat16 [8192], replicated
- w_gate: bfloat16 [8192, 24576], P(None, 'tp')
- w_up: bfloat16 [8192, 24576], P(None, 'tp')
- w_down: bfloat16 [24576, 8192], P('tp')
Outputs:
- output: bfloat16 [8, 512, 8192], P('dp'), parts along dimension 0
There are 2 independent parts. The reference program is written for one: setup_inputs(seed, part) draws one part's arguments, and reference() takes and returns one part's arrays. A program takes and returns all parts, laid end to end along the dimension named above; an argument that names none is the same for every part.
All inputs are finite; a program needn't handle non-finite values.
Results may differ from the reference program's by a relative error of at most 0.017.
Values are sent between devices in bfloat16 or wider.
A program may use at most 768 MiB of HBM per device.

```python
import jax
import jax.numpy as jnp
from jax import lax

SEQUENCES = 4
TOKENS = 512
D = 8192
HEADS = 64
KV_HEADS = 64
HEAD = 128
FF = 24576
THETA = 10000


def setup_inputs(seed: int = 0, part: int = 0) -> dict:
    kx, ka, km, kq, kk, kv, ko, kg, ku, kd = jax.random.split(jax.random.key(seed), 10)

    def weights(key, rows, columns):
        return jax.random.normal(key, (rows, columns), jnp.float32) * rows**-0.5

    drawn = {
        "x": jax.random.normal(jax.random.fold_in(kx, part), (SEQUENCES, TOKENS, D), jnp.float32),
        "gain_a": 1 + 0.1 * jax.random.normal(ka, (D,), jnp.float32),
        "wq": 2 * weights(kq, D, HEADS * HEAD),
        "wk": 2 * weights(kk, D, KV_HEADS * HEAD),
        "wv": 4 * weights(kv, D, KV_HEADS * HEAD),
        "wo": weights(ko, HEADS * HEAD, D),
        "gain_m": 1 + 0.1 * jax.random.normal(km, (D,), jnp.float32),
        "w_gate": weights(kg, D, FF),
        "w_up": weights(ku, D, FF),
        "w_down": 3 * weights(kd, FF, D),
    }
    return {k: v.astype(jnp.bfloat16) for k, v in drawn.items()}


def normed(x, gain):
    wide = x.astype(jnp.float32)
    scale = lax.rsqrt(jnp.mean(wide * wide, -1, keepdims=True) + 1e-6)
    return (wide * scale * gain.astype(jnp.float32)).astype(jnp.bfloat16)


def turned(t, place, theta):
    half = t.shape[-1] // 2
    angle = place.astype(jnp.float32)[:, None] * theta ** (-jnp.arange(half, dtype=jnp.float32) / half)
    cos, sin = jnp.cos(angle)[:, None], jnp.sin(angle)[:, None]
    a, b = t[..., :half].astype(jnp.float32), t[..., half:].astype(jnp.float32)
    return jnp.concatenate([a * cos - b * sin, b * cos + a * sin], -1).astype(jnp.bfloat16)


def matmul(a, w):
    return jnp.dot(a, w, preferred_element_type=jnp.float32).astype(jnp.bfloat16)


def einsum(form, a, b):
    return jnp.einsum(form, a.astype(jnp.float32), b.astype(jnp.float32))


def attention(q, k, v):
    scores = einsum("tgsd,ugd->gstu", q, k) * q.shape[-1] ** -0.5
    token = jnp.arange(q.shape[0])
    scores = jnp.where(token[:, None] >= token, scores, -jnp.inf)
    weights = jax.nn.softmax(scores, -1).astype(jnp.bfloat16)
    return einsum("gstu,ugd->tgsd", weights, v).astype(jnp.bfloat16)


def one(x, gain_a, wq, wk, wv, wo, gain_m, w_gate, w_up, w_down):
    rows = x.shape[0]
    a, place = normed(x, gain_a), jnp.arange(rows)
    k = turned(matmul(a, wk).reshape(rows, -1, HEAD), place, THETA)
    q = turned(matmul(a, wq).reshape(rows, -1, HEAD), place, THETA).reshape(rows, k.shape[1], -1, HEAD)
    v = matmul(a, wv).reshape(rows, -1, HEAD)
    seen = attention(q, k, v).reshape(rows, -1)
    h = (x.astype(jnp.float32) + jnp.dot(seen, wo, preferred_element_type=jnp.float32)).astype(jnp.bfloat16)
    b = normed(h, gain_m)
    gate = jnp.dot(b, w_gate, preferred_element_type=jnp.float32)
    up = jnp.dot(b, w_up, preferred_element_type=jnp.float32)
    hidden = (jax.nn.silu(gate) * up).astype(jnp.bfloat16)
    return (h.astype(jnp.float32) + jnp.dot(hidden, w_down, preferred_element_type=jnp.float32)).astype(jnp.bfloat16)


def reference(x, gain_a, wq, wk, wv, wo, gain_m, w_gate, w_up, w_down):
    return lax.map(lambda sequence: one(sequence, gain_a, wq, wk, wv, wo, gain_m, w_gate, w_up, w_down), x)
```

```python
import functools

import jax
import jax.numpy as jnp
from jax import lax
from jax.experimental import pallas as pl
from jax.experimental.pallas import tpu as pltpu
from jax.sharding import PartitionSpec as P

HEAD = 128
THETA = 10000
MESH = pl.DeviceIdType.MESH
ANY = pl.BlockSpec(memory_space=pl.ANY)
VMEM = 66_000_000
F32, BF16 = jnp.float32, jnp.bfloat16


def _dot(a, b):
    return jnp.dot(a, b, preferred_element_type=F32)


def _by_columns(width, fn, init=None, tile=1024):
    tile = min(tile, width)
    return lax.fori_loop(0, width // tile, lambda i, s: fn(pl.ds(pl.multiple_of(i * tile, tile), tile), s), init)


def _place():
    me, n = lax.axis_index("tp"), lax.axis_size("tp")
    chips = n // 2
    j, c = me // 2, me % 2
    r, l, o = (j + 1) % chips, (j + chips - 1) % chips, (j + 2) % chips
    return j, c, r, l, o, {"r": 2 * r + c, "l": 2 * l + c, "p": 2 * j + 1 - c}


def _greet():
    to = _place()[5]
    sem = pltpu.get_barrier_semaphore()
    for name in ("p", "l", "r"):
        pl.semaphore_signal(sem, inc=1, device_id={"tp": to[name]}, device_id_type=MESH)
    pl.semaphore_wait(sem, 3)


class Gather:
    copies = 10

    def __init__(self, own):
        self.inputs = [own]
        _, self.w, self.d = own.shape
        self.in_specs = [ANY]
        self.out_shape = [jax.ShapeDtypeStruct((2, 4, 2, self.w, self.d), BF16)]
        self.scratch = [pltpu.VMEM((2, self.w, self.d), BF16), pltpu.SemaphoreType.DMA((10,)), pltpu.SemaphoreType.DMA((10,)),
                        pltpu.SemaphoreType.DMA((2,))]

    def bind(self, ins, outs, scratch):
        (self.own,), (self.full,), (self.ov, self.ss, self.rs, self.ls) = ins, outs, scratch

    def cp(self, k):
        j, c, r, l, o, to = _place()
        full, ov = self.full, self.ov
        src, dst, dev = [
            lambda: (ov.at[0], full.at[c, j, 0], "r"),
            lambda: (ov.at[1], full.at[c, j, 1], "r"),
            lambda: (ov.at[1], full.at[c, j, 1], "l"),
            lambda: (ov.at[0], full.at[c, j, 0], "l"),
            lambda: (full.at[c, l, 0], full.at[c, l, 0], "r"),
            lambda: (full.at[c, r, 1], full.at[c, r, 1], "l"),
            lambda: (ov, full.at[c, j], "p"),
            lambda: (full.at[c, l], full.at[c, l], "p"),
            lambda: (full.at[c, r], full.at[c, r], "p"),
            lambda: (full.at[c, o], full.at[c, o], "p"),
        ][k]()
        return pltpu.make_async_remote_copy(src_ref=src, dst_ref=dst, send_sem=self.ss.at[k], recv_sem=self.rs.at[k],
                                            device_id={"tp": to[dev]}, device_id_type=MESH)

    def load(self):
        return pltpu.make_async_copy(self.own, self.ov, self.ls.at[0])

    def store(self):
        j, c = _place()[:2]
        return pltpu.make_async_copy(self.ov, self.full.at[c, j], self.ls.at[1])

    def early(self):
        self.load().start()

    def t0(self):
        self.load().wait()
        for k in (0, 2, 1, 3, 6):
            self.cp(k).start()
        self.store().start()

    def t1(self):
        self.cp(0).wait_recv()
        self.cp(4).start()
        self.cp(2).wait_recv()
        self.cp(5).start()

    def t2(self):
        self.cp(1).wait_recv()
        self.cp(7).start()
        self.cp(3).wait_recv()
        self.cp(8).start()

    def t3(self):
        self.cp(4).wait_recv()
        self.cp(5).wait_recv()
        self.cp(9).start()

    def t4(self):
        for k in (6, 7, 8, 9):
            self.cp(k).wait_recv()
        for k in range(10):
            self.cp(k).wait_send()
        self.store().wait()

    def ticks(self, at):
        return list(zip(at, (self.t0, self.t1, self.t2, self.t3, self.t4)))


class Scatter:
    def __init__(self, own, other, residual, chunk=None, gain=None):
        self.inputs = [own, other, residual] + ([] if gain is None else [gain])
        _, _, self.w, self.d = own.shape
        self.chunk, self.normed = chunk, gain is not None
        self.in_specs = [ANY, ANY, ANY] + ([] if gain is None else [pl.BlockSpec(memory_space=pltpu.VMEM)])
        rows = jax.ShapeDtypeStruct((2, self.w, self.d), BF16)
        self.out_shape = [rows] * (2 if self.normed else 1)
        w, d = self.w, self.d
        self.scratch = [pltpu.VMEM((4, 2, w, d), BF16), pltpu.VMEM((4, w, d), F32), pltpu.VMEM((6, w, d), BF16), pltpu.VMEM((2, w, d), BF16),
                        pltpu.VMEM((4, w, d), BF16), pltpu.SemaphoreType.DMA((7,)), pltpu.SemaphoreType.DMA((7,)),
                        pltpu.SemaphoreType.DMA((7,))]

    def bind(self, ins, outs, scratch):
        self.own, self.other, self.res = ins[:3]
        self.gain = ins[3] if self.normed else None
        self.outs = outs
        self.r0, self.f, self.stg, self.a1, self.a2, self.ss, self.rs, self.ls = scratch

    def cp(self, k):
        to = _place()[5]
        stg = self.stg
        src, dst, dev = [
            lambda: (self.other, self.r0, "p"),
            lambda: (stg.at[0], self.a1.at[0], "r"),
            lambda: (stg.at[1], self.a1.at[1], "l"),
            lambda: (stg.at[2], self.a2.at[1], "r"),
            lambda: (stg.at[3], self.a2.at[2], "l"),
            lambda: (stg.at[4], self.a2.at[0], "r"),
            lambda: (stg.at[5], self.a2.at[3], "l"),
        ][k]()
        return pltpu.make_async_remote_copy(src_ref=src, dst_ref=dst, send_sem=self.ss.at[k], recv_sem=self.rs.at[k],
                                            device_id={"tp": to[dev]}, device_id_type=MESH)

    def first(self, i):
        j, c, r, l, o, _ = _place()
        at = ((o, 0), (o, 1), (r, 1), (l, 0))[i]
        return pltpu.make_async_copy(self.own.at[at], self.f.at[i], self.ls.at[i])

    def second(self, i):
        j, c, r, l, o, _ = _place()
        at = ((r, 0), (l, 1), (j, 0), (j, 1))[i]
        return pltpu.make_async_copy(self.own.at[at], self.f.at[i], self.ls.at[i])

    def residual(self):
        j, c, r, l, o, _ = _place()
        src = self.res if self.chunk is None else self.res.at[self.chunk, c, j]
        return pltpu.make_async_copy(src, self.r0.at[o], self.ls.at[4])

    def out(self, i):
        return pltpu.make_async_copy(self.stg.at[pl.ds(2 * i, 2)], self.outs[i], self.ls.at[5 + i])

    def add(self, to, f, *terms):
        def piece(cols, _):
            total = self.f[f, :, cols]
            for ref, at in terms:
                total = total + ref[(*at, slice(None), cols)].astype(F32)
            self.stg[to, :, cols] = total.astype(BF16)

        _by_columns(self.d, piece)

    def early(self):
        for i in range(4):
            self.first(i).start()

    def t0(self):
        self.cp(0).start()

    def t1(self):
        j, c, r, l, o, _ = _place()
        for i in range(4):
            self.first(i).wait()
        self.cp(0).wait_recv()
        self.add(0, 0, (self.r0, (o, 0)))
        self.add(1, 1, (self.r0, (o, 1)))
        self.residual().start()
        self.second(0).start()
        self.second(1).start()
        self.cp(1).start()
        self.cp(2).start()
        self.add(2, 2, (self.r0, (r, 1)))
        self.add(3, 3, (self.r0, (l, 0)))
        self.second(2).start()
        self.second(3).start()
        self.cp(3).start()
        self.cp(4).start()

    def t2(self):
        j, c, r, l, o, _ = _place()
        self.second(0).wait()
        self.second(1).wait()
        self.cp(1).wait_recv()
        self.add(4, 0, (self.r0, (r, 0)), (self.a1, (0,)))
        self.cp(2).wait_recv()
        self.cp(5).start()
        self.add(5, 1, (self.r0, (l, 1)), (self.a1, (1,)))
        self.residual().wait()
        self.cp(6).start()

    def t3(self):
        j, c, r, l, o, _ = _place()
        self.second(2).wait()
        self.second(3).wait()
        for k in (3, 4, 5, 6):
            self.cp(k).wait_recv()
        for k in (1, 2, 3, 4):
            self.cp(k).wait_send()
        for half in range(2):

            def piece(cols, squares):
                sums = self.f[2 + half, :, cols] + self.r0[j, half, :, cols].astype(F32)
                sums = sums + self.a2[half, :, cols].astype(F32) + self.a2[2 + half, :, cols].astype(F32)
                h = (self.r0[o, half, :, cols].astype(F32) + sums).astype(BF16)
                self.stg[half, :, cols] = h
                wide = h.astype(F32)
                return squares + jnp.sum(wide * wide, -1, keepdims=True) if self.normed else squares

            squares = _by_columns(self.d, piece, jnp.zeros((self.w, 1), F32))
            if self.normed:
                scale = lax.rsqrt(squares / self.d + 1e-6)

                def turn(cols, _):
                    self.stg[2 + half, :, cols] = (self.stg[half, :, cols].astype(F32) * scale * self.gain[:, cols].astype(F32)).astype(BF16)

                _by_columns(self.d, turn)
        for i in range(len(self.outs)):
            self.out(i).start()

    def t4(self):
        for i in range(len(self.outs)):
            self.out(i).wait()
        for k in (0, 5, 6):
            self.cp(k).wait_send()

    def ticks(self, at):
        return list(zip(at, (self.t0, self.t1, self.t2, self.t3, self.t4)))


def _norm_rows(ref, gain_ref, group=16):
    rows, d = ref.shape

    def some(i, _):
        at = pl.ds(pl.multiple_of(i * group, group), group)

        def square(cols, s):
            wide = ref[at, cols].astype(F32)
            return s + wide * wide

        tile = min(1024, d)
        squares = jnp.sum(_by_columns(d, square, jnp.zeros((group, tile), F32)), -1, keepdims=True)
        scale = lax.rsqrt(squares / d + 1e-6)

        def turn(cols, _):
            ref[at, cols] = (ref[at, cols].astype(F32) * scale * gain_ref[:, cols].astype(F32)).astype(BF16)

        _by_columns(d, turn)

    lax.fori_loop(0, rows // group, some, None)


def _split(acc, own_ref, other_ref):
    c = lax.axis_index("tp") % 2
    half = acc.shape[0] // 2
    top, low = acc[:half], acc[half:]
    own_ref[...] = jnp.where(c == 0, top, low).reshape(own_ref.shape)
    other_ref[...] = jnp.where(c == 0, low, top).astype(BF16).reshape(other_ref.shape)


class Attention:
    def __init__(self, chunk, x, gain, cs, sn, wq, wk, wv, wo):
        _, self.rows, d = x.shape
        width = wq.shape[1]
        self.chunk, self.d = chunk, d
        self.tile = tile = min(256, width)
        self.nq = nq = width // tile
        self.out = out = min(1024, d)
        self.nw = nw = d // out
        whole = pl.BlockSpec(memory_space=pltpu.VMEM)
        w_spec = pl.BlockSpec((d, tile), lambda s: (0, jnp.minimum(s, nq - 1)))
        back = lambda s: jnp.maximum(s - 2 * nq, 0)
        w = self.rows // 16
        self.inputs = [x, gain, cs, sn, wq, wk, wv, wo]
        self.in_specs = [ANY, whole, whole, whole, w_spec, w_spec, w_spec, pl.BlockSpec((width, out), lambda s: (0, back(s)))]
        self.out_shape = [jax.ShapeDtypeStruct((4, 2, w, d), F32), jax.ShapeDtypeStruct((4, 2, w, d), BF16)]
        self.out_specs = [pl.BlockSpec((4, 2, w, out), lambda s: (0, 0, 0, back(s)))] * 2
        qkv = pltpu.VMEM((nq, self.rows, tile), BF16)
        self.scratch = [pltpu.VMEM((self.rows, d), BF16), qkv, qkv, qkv, pltpu.VMEM((self.rows, width), BF16), pltpu.SemaphoreType.DMA(())]
        self.times = [8 + 7.2 * i for i in range(nq)] + [8 + 7.2 * nq + 2.0 * i for i in range(nq)]
        self.times += [8 + 9.2 * nq + 1.2 * i for i in range(nw)]
        self.times[0] = 0
        self.flops = 2 * self.rows * d * width * 4

    def bind(self, ins, outs, scratch):
        self.x, self.gain, self.cs, self.sn, self.wq, self.wk, self.wv, self.wo = ins
        self.own, self.other = outs
        self.a, self.q, self.k, self.v, self.seen, self.sem = scratch

    def early(self):
        pltpu.make_async_copy(self.x.at[self.chunk], self.a, self.sem).start()

    def begin(self):
        pltpu.make_async_copy(self.x.at[self.chunk], self.a, self.sem).wait()
        _norm_rows(self.a, self.gain)

    def step(self, s):
        nq, tile = self.nq, self.tile

        @pl.when(s < nq)
        def _():
            for w, to in ((self.wq, self.q), (self.wk, self.k), (self.wv, self.v)):
                to[s] = _dot(self.a[...], w[...]).astype(BF16)

        @pl.when((s >= nq) & (s < 2 * nq))
        def _():
            t = s - nq
            cs, sn = self.cs[...], self.sn[...]
            rows = self.rows
            bq = min(256, rows)

            def turned(ref, h):
                wide = ref[t, :, h : h + HEAD].astype(F32)
                return (wide * cs + pltpu.roll(wide, HEAD // 2, 1) * sn).astype(BF16)

            done = []
            for h in range(0, tile, HEAD):
                q, k, v = turned(self.q, h), turned(self.k, h), self.v[t, :, h : h + HEAD]
                parts = []
                for at in range(0, rows, bq):
                    end = at + bq
                    scores = lax.dot_general(q[at:end], k[:end], (((1,), (1,)), ((), ())), preferred_element_type=F32) * HEAD**-0.5
                    ok = lax.broadcasted_iota(jnp.int32, (bq, end), 0) + at >= lax.broadcasted_iota(jnp.int32, (bq, end), 1)
                    scores = jnp.where(ok, scores, -1e30)
                    p = jnp.exp(scores - scores.max(-1, keepdims=True))
                    total = p.sum(-1, keepdims=True)
                    parts.append(_dot(p.astype(BF16), v[:end]) * (1 / total))
                done.append(jnp.concatenate(parts, 0).astype(BF16))
            self.seen[:, pl.ds(pl.multiple_of(t * tile, tile), tile)] = jnp.concatenate(done, 1)

        @pl.when(s >= 2 * nq)
        def _():
            _split(_dot(self.seen[...], self.wo[...]), self.own, self.other)


class Mlp:
    def __init__(self, b, w_gate, w_up, w_down):
        self.rows, d = b.shape
        ff = w_gate.shape[1]
        self.tile = tile = min(256, ff)
        self.ng = ng = ff // tile
        self.out = out = min(512, d)
        nd = d // out
        w_spec = pl.BlockSpec((d, tile), lambda s: (0, jnp.minimum(s, ng - 1)))
        back = lambda s: jnp.maximum(s - ng, 0)
        w = self.rows // 16
        self.inputs = [b, w_gate, w_up, w_down]
        self.in_specs = [pl.BlockSpec((self.rows, d), lambda s: (0, 0), pipeline_mode=pl.Buffered(1)), w_spec, w_spec,
                         pl.BlockSpec((ff, out), lambda s: (0, back(s)))]
        self.out_shape = [jax.ShapeDtypeStruct((4, 2, w, d), F32), jax.ShapeDtypeStruct((4, 2, w, d), BF16)]
        self.out_specs = [pl.BlockSpec((4, 2, w, out), lambda s: (0, 0, 0, back(s)))] * 2
        self.scratch = [pltpu.VMEM((self.rows, ff), BF16)]
        self.times = [4.7 * i for i in range(ng)] + [4.7 * ng + 1.8 * i for i in range(nd)]
        self.flops = 2 * self.rows * d * ff * 3

    def bind(self, ins, outs, scratch):
        self.b, self.wg, self.wu, self.wd = ins
        self.own, self.other = outs
        (self.hidden,) = scratch

    def early(self):
        pass

    begin = early

    def step(self, s):
        @pl.when(s < self.ng)
        def _():
            b = self.b[...]
            gate = _dot(b, self.wg[...])
            up = _dot(b, self.wu[...])
            self.hidden[:, pl.ds(pl.multiple_of(s * self.tile, self.tile), self.tile)] = (gate * jax.nn.sigmoid(gate) * up).astype(BF16)

        @pl.when(s >= self.ng)
        def _():
            _split(_dot(self.hidden[...], self.wd[...]), self.own, self.other)


class Nothing:
    inputs = in_specs = out_shape = out_specs = scratch = []
    times, flops = [0], 0

    def bind(self, *_):
        pass

    early = begin = step = lambda self, *_: None


def run(work, jobs, number, name):
    steps = len(work.times)
    parts = [work] + [j for j, _ in jobs]

    def body(*refs):
        refs = list(refs)
        take = lambda n: [refs.pop(0) for _ in range(n)]
        ins = [take(len(p.inputs)) for p in parts]
        outs = [take(len(p.out_shape)) for p in parts]
        scratch = [take(len(p.scratch)) for p in parts]
        for p, i, o, s in zip(parts, ins, outs, scratch):
            p.bind(i, o, s)
        s = pl.program_id(0)
        ticks = sorted([t for job, at in jobs for t in job.ticks(at)], key=lambda t: t[0])
        places = {}
        for when, fn in ticks:
            later = [i for i, t in enumerate(work.times) if t >= when]
            places.setdefault(later[0] if later else steps, []).append(fn)

        @pl.when(s == 0)
        def _():
            for p in parts:
                p.early()
            if jobs:
                _greet()
            for fn in places.pop(0, []):
                fn()
            work.begin()

        end = places.pop(steps, [])
        for i, fns in places.items():

            @pl.when(s == i)
            def _(fns=fns):
                for fn in fns:
                    fn()

        work.step(s)
        if end:

            @pl.when(s == steps - 1)
            def _():
                for fn in end:
                    fn()

    shapes = [x for p in parts for x in p.out_shape]
    specs = list(work.out_specs) + [ANY] * (len(shapes) - len(work.out_specs))
    got = pl.pallas_call(
        body,
        grid=(steps,),
        in_specs=[x for p in parts for x in p.in_specs],
        out_specs=specs,
        out_shape=shapes,
        scratch_shapes=[x for p in parts for x in p.scratch],
        compiler_params=pltpu.CompilerParams(dimension_semantics=("arbitrary",), vmem_limit_bytes=VMEM, has_side_effects=bool(jobs),
                                             collective_id=number if jobs else None),
        name=name,
    )(*[x for p in parts for x in p.inputs])
    got = list(got)
    return [[got.pop(0) for _ in p.out_shape] for p in parts]


def solution(mesh):
    def step(x, gain_a, wq, wk, wv, wo, gain_m, w_gate, w_up, w_down):
        batch, rows, d = x.shape
        half = HEAD // 2
        angle = jnp.arange(rows, dtype=F32)[:, None] * THETA ** (-jnp.arange(half, dtype=F32) / half)
        cos, sin = jnp.cos(angle), jnp.sin(angle)
        cs, sn = jnp.concatenate([cos, cos], 1), jnp.concatenate([-sin, sin], 1)
        gain_a, gain_m = gain_a.reshape(1, d), gain_m.reshape(1, d)
        pieces = x.reshape(batch, 2, 4, 2, rows // 16, d)
        attention = lambda c: Attention(c, x, gain_a, cs, sn, wq, wk, wv, wo)
        mlp = lambda c: Mlp(b[c].reshape(rows, d), w_gate, w_up, w_down)
        first = lambda c: Scatter(*p1[c], pieces, c, gain_m)
        second = lambda c: Scatter(*p2[c], h[c])
        p1, p2, h, b, own_b, own_y, y = {}, {}, {}, {}, {}, {}, {}
        both = ((0, 15, 26, 60, 1000), (0, 9, 37, 71, 1001))

        (p1[0],) = run(attention(0), [], 0, "a0")
        p1[1], (h[0], own_b[0]) = run(attention(1), [(first(0), (0, 9, 25, 46, 1000))], 1, "a1")
        p1[2], (b[0],), (h[1], own_b[1]) = run(attention(2), [(Gather(own_b[0]), both[0]), (first(1), both[1])], 2, "a2")
        p1[3], (b[1],), (h[2], own_b[2]) = run(attention(3), [(Gather(own_b[1]), both[0]), (first(2), both[1])], 3, "a3")
        p2[0], (b[2],), (h[3], own_b[3]) = run(mlp(0), [(Gather(own_b[2]), both[0]), (first(3), both[1])], 4, "m0")
        p2[1], (b[3],), (own_y[0],) = run(mlp(1), [(Gather(own_b[3]), both[0]), (second(0), both[1])], 5, "m1")
        p2[2], (y[0],), (own_y[1],) = run(mlp(2), [(Gather(own_y[0]), both[0]), (second(1), both[1])], 6, "m2")
        p2[3], (y[1],), (own_y[2],) = run(mlp(3), [(Gather(own_y[1]), both[0]), (second(2), both[1])], 7, "m3")
        _, (y[2],), (own_y[3],) = run(Nothing(), [(Gather(own_y[2]), both[0]), (second(3), both[1])], 8, "t1")
        _, (y[3],) = run(Nothing(), [(Gather(own_y[3]), both[0])], 9, "t2")
        return jnp.stack([y[c].reshape(rows, d) for c in range(batch)])

    tokens, whole, columns, rows_of = P("dp", None, None), P(None), P(None, "tp"), P("tp", None)
    return jax.shard_map(
        step,
        mesh=mesh,
        in_specs=(tokens, whole, columns, columns, columns, rows_of, whole, columns, columns, rows_of),
        out_specs=tokens,
        check_vma=False,
    )
```

```python
import functools

import jax
import jax.numpy as jnp
from jax import lax
from jax.experimental import pallas as pl
from jax.experimental.pallas import tpu as pltpu
from jax.sharding import PartitionSpec as P

HEAD = 128
THETA = 10000
MESH = pl.DeviceIdType.MESH
ANY = pl.BlockSpec(memory_space=pl.ANY)
VMEM = 66_000_000
F32, BF16 = jnp.float32, jnp.bfloat16


def _dot(a, b):
    return jnp.dot(a, b, preferred_element_type=F32)


def _by_columns(width, fn, init=None, tile=1024):
    tile = min(tile, width)
    return lax.fori_loop(0, width // tile, lambda i, s: fn(pl.ds(pl.multiple_of(i * tile, tile), tile), s), init)


def _place():
    me, n = lax.axis_index("tp"), lax.axis_size("tp")
    chips = n // 2
    j, c = me // 2, me % 2
    r, l, o = (j + 1) % chips, (j + chips - 1) % chips, (j + 2) % chips
    return j, c, r, l, o, {"r": 2 * r + c, "l": 2 * l + c, "p": 2 * j + 1 - c}


def _greet():
    to = _place()[5]
    sem = pltpu.get_barrier_semaphore()
    for name in ("p", "l", "r"):
        pl.semaphore_signal(sem, inc=1, device_id={"tp": to[name]}, device_id_type=MESH)
    pl.semaphore_wait(sem, 3)


class Gather:
    def __init__(self, own=None, after=None):
        self.inputs = [] if own is None else [own]
        self.after = after
        self.w, self.d = own.shape[1:] if after is None else (after.w, after.d)
        self.in_specs = [ANY] * len(self.inputs)
        self.out_shape = [jax.ShapeDtypeStruct((2, 4, 2, self.w, self.d), BF16)]
        self.scratch = [pltpu.VMEM((2, self.w, self.d), BF16), pltpu.SemaphoreType.DMA((10,)), pltpu.SemaphoreType.DMA((10,)),
                        pltpu.SemaphoreType.DMA((2,))]

    def bind(self, ins, outs, scratch):
        (self.own,) = ins if self.after is None else self.after.outs[-1:]
        (self.full,), (self.ov, self.ss, self.rs, self.ls) = outs, scratch

    def cp(self, k):
        j, c, r, l, o, to = _place()
        full, ov = self.full, self.ov
        src, dst, dev = [
            lambda: (ov.at[0], full.at[c, j, 0], "r"),
            lambda: (ov.at[1], full.at[c, j, 1], "r"),
            lambda: (ov.at[1], full.at[c, j, 1], "l"),
            lambda: (ov.at[0], full.at[c, j, 0], "l"),
            lambda: (full.at[c, l, 0], full.at[c, l, 0], "r"),
            lambda: (full.at[c, r, 1], full.at[c, r, 1], "l"),
            lambda: (ov, full.at[c, j], "p"),
            lambda: (full.at[c, l], full.at[c, l], "p"),
            lambda: (full.at[c, r], full.at[c, r], "p"),
            lambda: (full.at[c, o], full.at[c, o], "p"),
        ][k]()
        return pltpu.make_async_remote_copy(src_ref=src, dst_ref=dst, send_sem=self.ss.at[k], recv_sem=self.rs.at[k],
                                            device_id={"tp": to[dev]}, device_id_type=MESH)

    def load(self):
        return pltpu.make_async_copy(self.own, self.ov, self.ls.at[0])

    def store(self):
        j, c = _place()[:2]
        return pltpu.make_async_copy(self.ov, self.full.at[c, j], self.ls.at[1])

    def early(self):
        if self.after is None:
            self.load().start()

    def t0(self):
        if self.after is not None:
            self.load().start()
        self.load().wait()
        for k in (0, 2, 6):
            self.cp(k).start()
        self.store().start()

    def rest(self):
        self.cp(1).start()
        self.cp(3).start()

    def t1(self):
        self.cp(0).wait_recv()
        self.cp(4).start()
        self.cp(2).wait_recv()
        self.cp(5).start()

    def t2(self):
        self.cp(1).wait_recv()
        self.cp(7).start()
        self.cp(3).wait_recv()
        self.cp(8).start()

    def t3(self):
        self.cp(4).wait_recv()
        self.cp(5).wait_recv()
        self.cp(9).start()

    def t4(self):
        for k in (6, 7, 8, 9):
            self.cp(k).wait_recv()
        for k in range(10):
            self.cp(k).wait_send()
        self.store().wait()

    def ticks(self, at):
        return list(zip(at, (self.t0, self.rest, self.t1, self.t2, self.t3, self.t4)))


class Scatter:
    def __init__(self, own, other, residual, chunk=None, gain=None):
        self.inputs = [own, other, residual] + ([] if gain is None else [gain])
        _, _, self.w, self.d = own.shape
        self.chunk, self.normed = chunk, gain is not None
        self.in_specs = [ANY, ANY, ANY] + ([] if gain is None else [pl.BlockSpec(memory_space=pltpu.VMEM)])
        rows = jax.ShapeDtypeStruct((2, self.w, self.d), BF16)
        self.out_shape = [rows] * (2 if self.normed else 1)
        w, d = self.w, self.d
        self.scratch = [pltpu.VMEM((4, 2, w, d), BF16), pltpu.VMEM((4, w, d), F32), pltpu.VMEM((6, w, d), BF16), pltpu.VMEM((2, w, d), BF16),
                        pltpu.VMEM((4, w, d), BF16), pltpu.SemaphoreType.DMA((10,)), pltpu.SemaphoreType.DMA((10,)),
                        pltpu.SemaphoreType.DMA((7,))]

    def bind(self, ins, outs, scratch):
        self.own, self.other, self.res = ins[:3]
        self.gain = ins[3] if self.normed else None
        self.outs = outs
        self.r0, self.f, self.stg, self.a1, self.a2, self.ss, self.rs, self.ls = scratch

    def cp(self, k):
        j, c, r, l, o, to = _place()
        stg = self.stg
        src, dst, dev = [
            lambda: (self.other.at[o], self.r0.at[o], "p"),
            lambda: (stg.at[0], self.a1.at[0], "r"),
            lambda: (stg.at[1], self.a1.at[1], "l"),
            lambda: (stg.at[2], self.a2.at[1], "r"),
            lambda: (stg.at[3], self.a2.at[2], "l"),
            lambda: (stg.at[4], self.a2.at[0], "r"),
            lambda: (stg.at[5], self.a2.at[3], "l"),
            lambda: (self.other.at[r], self.r0.at[r], "p"),
            lambda: (self.other.at[l], self.r0.at[l], "p"),
            lambda: (self.other.at[j], self.r0.at[j], "p"),
        ][k]()
        return pltpu.make_async_remote_copy(src_ref=src, dst_ref=dst, send_sem=self.ss.at[k], recv_sem=self.rs.at[k],
                                            device_id={"tp": to[dev]}, device_id_type=MESH)

    def first(self, i):
        j, c, r, l, o, _ = _place()
        at = ((o, 0), (o, 1), (r, 1), (l, 0))[i]
        return pltpu.make_async_copy(self.own.at[at], self.f.at[i], self.ls.at[i])

    def second(self, i):
        j, c, r, l, o, _ = _place()
        at = ((r, 0), (l, 1), (j, 0), (j, 1))[i]
        return pltpu.make_async_copy(self.own.at[at], self.f.at[i], self.ls.at[i])

    def residual(self):
        j, c, r, l, o, _ = _place()
        src = self.res if self.chunk is None else self.res.at[self.chunk, c, j]
        return pltpu.make_async_copy(src, self.r0.at[o], self.ls.at[4])

    def out(self, i):
        return pltpu.make_async_copy(self.stg.at[pl.ds(2 * i, 2)], self.outs[i], self.ls.at[5 + i])

    def add(self, to, f, *terms):
        def piece(cols, _):
            total = self.f[f, :, cols]
            for ref, at in terms:
                total = total + ref[(*at, slice(None), cols)].astype(F32)
            self.stg[to, :, cols] = total.astype(BF16)

        _by_columns(self.d, piece)

    def early(self):
        for i in range(4):
            self.first(i).start()

    def t0(self):
        for k in (0, 7, 8, 9):
            self.cp(k).start()

    def t1(self):
        j, c, r, l, o, _ = _place()
        for i in range(4):
            self.first(i).wait()
        self.cp(0).wait_recv()
        self.add(0, 0, (self.r0, (o, 0)))
        self.add(1, 1, (self.r0, (o, 1)))
        self.residual().start()
        self.second(0).start()
        self.second(1).start()
        self.cp(1).start()
        self.cp(2).start()
        self.cp(7).wait_recv()
        self.cp(8).wait_recv()
        self.add(2, 2, (self.r0, (r, 1)))
        self.add(3, 3, (self.r0, (l, 0)))
        self.second(2).start()
        self.second(3).start()
        self.cp(3).start()
        self.cp(4).start()

    def t2(self):
        j, c, r, l, o, _ = _place()
        self.second(0).wait()
        self.second(1).wait()
        self.cp(1).wait_recv()
        self.add(4, 0, (self.r0, (r, 0)), (self.a1, (0,)))
        self.cp(2).wait_recv()
        self.cp(5).start()
        self.add(5, 1, (self.r0, (l, 1)), (self.a1, (1,)))
        self.residual().wait()
        self.cp(6).start()

    def t3(self):
        j, c, r, l, o, _ = _place()
        self.second(2).wait()
        self.second(3).wait()
        for k in (9, 3, 4, 5, 6):
            self.cp(k).wait_recv()
        for k in (1, 2, 3, 4):
            self.cp(k).wait_send()
        for half in range(2):

            def piece(cols, squares):
                sums = self.f[2 + half, :, cols] + self.r0[j, half, :, cols].astype(F32)
                sums = sums + self.a2[half, :, cols].astype(F32) + self.a2[2 + half, :, cols].astype(F32)
                h = (self.r0[o, half, :, cols].astype(F32) + sums).astype(BF16)
                self.stg[half, :, cols] = h
                wide = h.astype(F32)
                return squares + jnp.sum(wide * wide, -1, keepdims=True) if self.normed else squares

            squares = _by_columns(self.d, piece, jnp.zeros((self.w, 1), F32))
            if self.normed:
                scale = lax.rsqrt(squares / self.d + 1e-6)

                def turn(cols, _):
                    self.stg[2 + half, :, cols] = (self.stg[half, :, cols].astype(F32) * scale * self.gain[:, cols].astype(F32)).astype(BF16)

                _by_columns(self.d, turn)
        for i in range(len(self.outs)):
            self.out(i).start()

    def t4(self):
        for i in range(len(self.outs)):
            self.out(i).wait()
        for k in (0, 5, 6, 7, 8, 9):
            self.cp(k).wait_send()

    def ticks(self, at):
        return list(zip(at, (self.t0, self.t1, self.t2, self.t3, self.t4)))


def _norm_rows(ref, gain_ref, group=16):
    rows, d = ref.shape

    def some(i, _):
        at = pl.ds(pl.multiple_of(i * group, group), group)

        tile = min(1024, d)
        columns = [slice(k, k + tile) for k in range(0, d, tile)]
        squares = jnp.zeros((group, tile), F32)
        for cols in columns:
            wide = ref[at, cols].astype(F32)
            squares = squares + wide * wide
        scale = lax.rsqrt(jnp.sum(squares, -1, keepdims=True) / d + 1e-6)
        for cols in columns:
            ref[at, cols] = (ref[at, cols].astype(F32) * scale * gain_ref[:, cols].astype(F32)).astype(BF16)

    lax.fori_loop(0, rows // group, some, None)


def _split(acc, own_ref, other_ref):
    c = lax.axis_index("tp") % 2
    half = acc.shape[0] // 2
    top, low = acc[:half], acc[half:]
    own_ref[...] = jnp.where(c == 0, top, low).reshape(own_ref.shape)
    other_ref[...] = jnp.where(c == 0, low, top).astype(BF16).reshape(other_ref.shape)


class Attention:
    def __init__(self, chunk, x, gain, cs, sn, wq, wk, wv, wo):
        _, self.rows, d = x.shape
        width = wq.shape[1]
        self.chunk, self.d = chunk, d
        self.tile = tile = min(256, width)
        self.nq = nq = width // tile
        self.out = out = min(1024, d)
        self.nw = nw = d // out
        whole = pl.BlockSpec(memory_space=pltpu.VMEM)
        w_spec = pl.BlockSpec((d, tile), lambda s: (0, jnp.minimum(s, nq - 1)))
        back = lambda s: jnp.maximum(s - 2 * nq, 0)
        w = self.rows // 16
        self.inputs = [x, gain, cs, sn, wq, wk, wv, wo]
        self.in_specs = [ANY, whole, whole, whole, w_spec, w_spec, w_spec, pl.BlockSpec((width, out), lambda s: (0, back(s)))]
        self.out_shape = [jax.ShapeDtypeStruct((4, 2, w, d), F32), jax.ShapeDtypeStruct((4, 2, w, d), BF16)]
        self.out_specs = [pl.BlockSpec((4, 2, w, out), lambda s: (0, 0, 0, back(s)))] * 2
        qkv = pltpu.VMEM((nq, self.rows, tile), BF16)
        self.scratch = [pltpu.VMEM((self.rows, d), BF16), qkv, qkv, qkv, pltpu.VMEM((self.rows, width), BF16), pltpu.SemaphoreType.DMA(())]
        self.times = [11 + 6.8 * i for i in range(nq)] + [11 + 6.8 * nq + 1.5 * i for i in range(nq)]
        self.times += [11 + 8.3 * nq + 1.2 * i for i in range(nw)]
        self.flops = 2 * self.rows * d * width * 4

    def bind(self, ins, outs, scratch):
        self.x, self.gain, self.cs, self.sn, self.wq, self.wk, self.wv, self.wo = ins
        self.own, self.other = outs
        self.a, self.q, self.k, self.v, self.seen, self.sem = scratch

    def early(self):
        pltpu.make_async_copy(self.x.at[self.chunk], self.a, self.sem).start()

    def begin(self):
        pltpu.make_async_copy(self.x.at[self.chunk], self.a, self.sem).wait()
        _norm_rows(self.a, self.gain)

    def step(self, s):
        nq, tile = self.nq, self.tile

        @pl.when(s < nq)
        def _():
            for w, to in ((self.wq, self.q), (self.wk, self.k), (self.wv, self.v)):
                to[s] = _dot(self.a[...], w[...]).astype(BF16)

        @pl.when((s >= nq) & (s < 2 * nq))
        def _():
            t = s - nq
            cs, sn = self.cs[...], self.sn[...]
            rows = self.rows
            bq = min(256, rows)

            def turned(ref, h):
                wide = ref[t, :, h : h + HEAD].astype(F32)
                return (wide * cs + pltpu.roll(wide, HEAD // 2, 1) * sn).astype(BF16)

            done = []
            for h in range(0, tile, HEAD):
                q, k, v = turned(self.q, h), turned(self.k, h), self.v[t, :, h : h + HEAD]
                parts = []
                for at in range(0, rows, bq):
                    end = at + bq
                    scores = lax.dot_general(q[at:end], k[:end], (((1,), (1,)), ((), ())), preferred_element_type=F32) * HEAD**-0.5
                    ok = lax.broadcasted_iota(jnp.int32, (bq, end), 0) + at >= lax.broadcasted_iota(jnp.int32, (bq, end), 1)
                    scores = jnp.where(ok, scores, -1e30)
                    p = jnp.exp(scores - scores.max(-1, keepdims=True))
                    total = p.sum(-1, keepdims=True)
                    parts.append(_dot(p.astype(BF16), v[:end]) * (1 / total))
                done.append(jnp.concatenate(parts, 0).astype(BF16))
            self.seen[:, pl.ds(pl.multiple_of(t * tile, tile), tile)] = jnp.concatenate(done, 1)

        @pl.when(s >= 2 * nq)
        def _():
            _split(_dot(self.seen[...], self.wo[...]), self.own, self.other)


class Mlp:
    def __init__(self, b, w_gate, w_up, w_down):
        self.rows, d = b.shape
        ff = w_gate.shape[1]
        self.tile = tile = min(256, ff)
        self.ng = ng = ff // tile
        self.out = out = min(1024, d)
        nd = d // out
        w_spec = pl.BlockSpec((d, tile), lambda s: (0, jnp.minimum(s, ng - 1)))
        back = lambda s: jnp.maximum(s - ng, 0)
        w = self.rows // 16
        self.inputs = [b, w_gate, w_up, w_down]
        self.in_specs = [ANY, w_spec, w_spec,
                         pl.BlockSpec((ff, out), lambda s: (0, back(s)))]
        self.out_shape = [jax.ShapeDtypeStruct((4, 2, w, d), F32), jax.ShapeDtypeStruct((4, 2, w, d), BF16)]
        self.out_specs = [pl.BlockSpec((4, 2, w, out), lambda s: (0, 0, 0, back(s)))] * 2
        self.scratch = [pltpu.VMEM((self.rows, ff), BF16), pltpu.VMEM((self.rows, d), BF16), pltpu.SemaphoreType.DMA(())]
        self.times = [5 + 4.6 * i for i in range(ng)] + [5 + 4.6 * ng + 3.6 * i for i in range(nd)]
        self.flops = 2 * self.rows * d * ff * 3

    def bind(self, ins, outs, scratch):
        self.b, self.wg, self.wu, self.wd = ins
        self.own, self.other = outs
        self.hidden, self.states, self.sem = scratch

    def early(self):
        pltpu.make_async_copy(self.b, self.states, self.sem).start()

    def begin(self):
        pltpu.make_async_copy(self.b, self.states, self.sem).wait()

    def step(self, s):
        @pl.when(s < self.ng)
        def _():
            b = self.states[...]
            gate = _dot(b, self.wg[...])
            up = _dot(b, self.wu[...])
            self.hidden[:, pl.ds(pl.multiple_of(s * self.tile, self.tile), self.tile)] = (gate * jax.nn.sigmoid(gate) * up).astype(BF16)

        @pl.when(s >= self.ng)
        def _():
            _split(_dot(self.hidden[...], self.wd[...]), self.own, self.other)


class Nothing:
    inputs = in_specs = out_shape = out_specs = scratch = []
    times, flops = [0], 0

    def bind(self, *_):
        pass

    early = begin = step = lambda self, *_: None


def run(work, jobs, number, name):
    steps = len(work.times)
    parts = [work] + [j for j, _ in jobs]

    def body(*refs):
        refs = list(refs)
        take = lambda n: [refs.pop(0) for _ in range(n)]
        ins = [take(len(p.inputs)) for p in parts]
        outs = [take(len(p.out_shape)) for p in parts]
        scratch = [take(len(p.scratch)) for p in parts]
        for p, i, o, s in zip(parts, ins, outs, scratch):
            p.bind(i, o, s)
        s = pl.program_id(0)
        ticks = sorted([t for job, at in jobs for t in job.ticks(at)], key=lambda t: t[0])
        places = {}
        for when, fn in ticks:
            later = [-1] if when <= 0 else [i for i, t in enumerate(work.times) if t >= when]
            places.setdefault(later[0] if later else steps, []).append(fn)

        @pl.when(s == 0)
        def _():
            for p in parts:
                p.early()
            if jobs:
                _greet()
            for fn in places.pop(-1, []):
                fn()
            work.begin()
            for fn in places.pop(0, []):
                fn()

        end = places.pop(steps, [])
        for i, fns in places.items():

            @pl.when(s == i)
            def _(fns=fns):
                for fn in fns:
                    fn()

        work.step(s)
        if end:

            @pl.when(s == steps - 1)
            def _():
                for fn in end:
                    fn()

    shapes = [x for p in parts for x in p.out_shape]
    specs = list(work.out_specs) + [ANY] * (len(shapes) - len(work.out_specs))
    got = pl.pallas_call(
        body,
        grid=(steps,),
        in_specs=[x for p in parts for x in p.in_specs],
        out_specs=specs,
        out_shape=shapes,
        scratch_shapes=[x for p in parts for x in p.scratch],
        compiler_params=pltpu.CompilerParams(dimension_semantics=("arbitrary",), vmem_limit_bytes=VMEM, has_side_effects=bool(jobs),
                                             collective_id=number if jobs else None),
        name=name,
    )(*[x for p in parts for x in p.inputs])
    got = list(got)
    return [[got.pop(0) for _ in p.out_shape] for p in parts]


def solution(mesh):
    def step(x, gain_a, wq, wk, wv, wo, gain_m, w_gate, w_up, w_down):
        batch, rows, d = x.shape
        half = HEAD // 2
        angle = jnp.arange(rows, dtype=F32)[:, None] * THETA ** (-jnp.arange(half, dtype=F32) / half)
        cos, sin = jnp.cos(angle), jnp.sin(angle)
        cs, sn = jnp.concatenate([cos, cos], 1), jnp.concatenate([-sin, sin], 1)
        gain_a, gain_m = gain_a.reshape(1, d), gain_m.reshape(1, d)
        pieces = x.reshape(batch, 2, 4, 2, rows // 16, d)
        attention = lambda c: Attention(c, x, gain_a, cs, sn, wq, wk, wv, wo)
        mlp = lambda c: Mlp(b[c].reshape(rows, d), w_gate, w_up, w_down)
        first = lambda c: Scatter(*p1[c], pieces, c, gain_m)
        second = lambda c: Scatter(*p2[c], h[c])
        p1, p2, h, b, own_b, own_y, y = {}, {}, {}, {}, {}, {}, {}
        scatter, gather = (0, 9.5, 29, 51, 1000), (0, 30.1, 30, 73, 62, 1001)
        chained, then = (0, 9.5, 26, 49, 54), (54.1, 54.2, 68, 79, 90, 1001)
        three, last = (0, 9.5, 29, 51, 55), (55.1, 55.2, 84, 94, 1002, 1003)

        (p1[0],) = run(attention(0), [], 0, "a0")
        p1[1], (h[0], own_b[0]) = run(attention(1), [(first(0), (0, 9.5, 26, 48, 1000))], 1, "a1")
        p1[2], (b[0],), (h[1], own_b[1]) = run(attention(2), [(Gather(own_b[0]), gather), (first(1), scatter)], 2, "a2")
        p1[3], (b[1],), (h[2], own_b[2]) = run(attention(3), [(Gather(own_b[1]), gather), (first(2), scatter)], 3, "a3")
        p2[0], (b[2],), (h[3], own_b[3]) = run(mlp(0), [(Gather(own_b[2]), gather), (first(3), scatter)], 4, "m0")
        p2[1], (b[3],), (own_y[0],) = run(mlp(1), [(Gather(own_b[3]), gather), (second(0), scatter)], 5, "m1")
        job = second(1)
        p2[2], (y[0],), _, (y[1],) = run(mlp(2), [(Gather(own_y[0]), gather), (job, three), (Gather(after=job), last)], 6, "m2")
        job = second(2)
        p2[3], _, (y[2],) = run(mlp(3), [(job, chained), (Gather(after=job), then)], 7, "m3")
        job = second(3)
        _, _, (y[3],) = run(Nothing(), [(job, chained), (Gather(after=job), then)], 8, "t1")
        return jnp.stack([y[c].reshape(rows, d) for c in range(batch)])

    tokens, whole, columns, rows_of = P("dp", None, None), P(None), P(None, "tp"), P("tp", None)
    return jax.shard_map(
        step,
        mesh=mesh,
        in_specs=(tokens, whole, columns, columns, columns, rows_of, whole, columns, columns, rows_of),
        out_specs=tokens,
        check_vma=False,
    )
```
